32 devices in a mesh: dp: 4 (over z), expert: 8 (over y, x, core).
Axes of the slice: x: 2, y: 2, z: 4, core: 2. Of those that a mesh axis runs over, the one named last changes fastest.
Arguments:
- tokens: bfloat16 [512, 7168], P('expert'), may hold values from -6 to 6
- routes: int32 [512, 8], P('expert'), may hold values from 0 to 7, all different within a row; in each aligned block of 64 rows (0 to 63, 64 to 127, ...) at most 64 rows name the same one
- route_weight: int32 [512, 8], P('expert'), may hold values from 1 to 4096
- w_gate: bfloat16 [8, 7168, 2048], P('expert', None, 'dp'), may hold values from -0.0625 to 0.0625
- w_up: bfloat16 [8, 7168, 2048], P('expert', None, 'dp'), may hold values from -0.0625 to 0.0625
- w_down: bfloat16 [8, 2048, 7168], P('expert', 'dp'), may hold values from -0.125 to 0.125
- prev_inputs: bfloat16 [4, 8, 64, 7168], P('dp', 'expert'), may hold values from -6 to 6
Outputs:
- mixed: bfloat16 [512, 7168], P('expert', 'dp')
- hessian: float32 [7168, 8, 128], P('dp', 'expert')
The draws below stay inside these ranges and needn't reach their ends.
Inputs may be any that keep to these rules, and one draw needn't show every extreme that they name: `routes`: in each aligned block of 64 rows (the rows of one index of expert) no expert is named more than 64 times, a bound that some block reaches; the 8 experts of a token differ.
All inputs are finite; a program needn't handle non-finite values.
Results may differ from the reference program's by a relative error of at most 0.014.
Values may be sent and summed in bfloat16 or wider, within the bound.
No kernel may reach another device: no remote copies, remote signals or barrier semaphores. Data moves between devices by JAX's collectives and lax.ppermute only.
A program may use at most 128 MiB of HBM per device.

```python
import math
import jax
import jax.numpy as jnp
import numpy as np
from jax import lax

D = 7168
FF = 2048
TOP = 8
TOK_DEV = 64
PREV_ROWS = 64
HESS_COLS = 128
EXPERTS = 8
TOKENS = 512
CAP = 64
N_DP = 4
N_EXPERT = 8


def with_ends(result, rng, smallest, largest):
    shape = result.shape
    spot = [jax.random.randint(jax.random.fold_in(rng, axis), (), 0, shape[axis]) for axis in range(len(shape))]
    result = result.at[tuple(spot)].set(smallest)
    longest = shape.index(max(shape))
    spot[longest] = (spot[longest] + 1) % shape[longest]
    return result.at[tuple(spot)].set(largest)


def block_scale(rng, extent, pieces, low, top_value):
    def one(position, blocks):
        steps = jax.random.uniform(jax.random.fold_in(jax.random.fold_in(rng, 6), position), (blocks,), jnp.float32, low / len(pieces), top_value / len(pieces))
        return jnp.repeat(jnp.exp(steps), extent[position] // blocks).reshape((-1,) + (1,) * (len(extent) - position - 1))

    level = one(*pieces[0])
    for cut in pieces[1:]:
        level = level * one(*cut)
    return level


def shared_out(own_key, own, number, rows, number_of, top, bound, skew):
    order = jax.random.permutation(own_key, number_of)
    crowded, usual = load_shares(number_of, rows * top, bound, skew, True), load_shares(number_of, rows * top, bound, skew, False)
    places = jnp.arange(number_of)

    def named(lengths, offset_by):
        used = int((lengths > 0).sum())
        fixed = max(1, used // 4)
        moved = fixed + (places - fixed + offset_by * (used - fixed)) % max(1, number_of - fixed)
        return jnp.zeros((number_of,), jnp.int32).at[order[jnp.where(places < fixed, places, moved)]].set(jnp.asarray(lengths, jnp.int32))

    lengths = jnp.where(number % 4 == 0, named(crowded, number // 4), named(usual, number - number // 4 - 1))
    mixed = jax.random.permutation(jax.random.fold_in(own, 3), number_of)
    giver, sink = mixed[0:number_of // 2 * 2:2], mixed[1:number_of // 2 * 2:2]
    margin = jnp.minimum(lengths[giver] - 1, bound - lengths[sink]) // 2
    margin = jnp.where((giver == order[0]) | (sink == order[0]) | (lengths[sink] == 0), 0, jnp.maximum(margin, 0))
    moved = jax.random.randint(jax.random.fold_in(own, 4), (number_of // 2,), 0, 1 << 20) % (margin + 1)
    lengths = lengths.at[giver].add(-moved).at[sink].add(moved)
    labels = jnp.searchsorted(jnp.cumsum(lengths), jnp.arange(rows * top), side="right").astype(jnp.int32)
    listing = labels.reshape(top, rows).T
    listing = listing[jax.random.permutation(jax.random.fold_in(own, 1), rows)]
    offset_by = jax.random.randint(jax.random.fold_in(own, 2), (rows, 1), 0, top)
    return jnp.take_along_axis(listing, (jnp.arange(top)[None, :] + offset_by) % top, axis=1)


def load_shares(amount, total, reach, lean, full):
    portions = [(1 << 20) // math.isqrt(grade ** lean) + 1 for grade in range(1, amount + 1)]
    largest = reach if full else min(reach, max(-(-total // amount), total * portions[0] // sum(portions)))
    least = 1 if total - largest >= amount - 1 else 0
    holding, surplus = [largest] + [least] * (amount - 1), total - largest - least * (amount - 1)
    while surplus > 0:
        candidates = [i for i in range(1, amount) if holding[i] < largest] or [i for i in range(1, amount) if holding[i] < reach]
        pool, budget = sum([portions[i] for i in candidates]), surplus
        for i in candidates:
            addition = min(reach - holding[i], max(1, budget * portions[i] // pool), surplus)
            holding[i] = holding[i] + addition
            surplus = surplus - addition
    return np.array(holding)


def centred(key, extent, width, most, shards=(), held_as=jnp.bfloat16):
    gain = block_scale(key, extent, shards, -0.22, 0.18) if shards else 1.0
    values = jax.random.normal(key, extent, jnp.float32) * width * gain
    return jnp.minimum(jnp.maximum(values, -most), most).astype(held_as)


def setup_inputs(seed: int = 0) -> dict:
    keys = jax.random.split(jax.random.key(seed), 8)
    tokens = centred(keys[0], (TOKENS, D), 1.0, 6.0, ((0, 8),))
    routes_keys = jax.random.split(jax.random.fold_in(keys[1], 1), TOKENS // TOK_DEV)
    routes_turns = jax.random.permutation(jax.random.fold_in(keys[1], 3), TOKENS // TOK_DEV)
    routes = jax.vmap(lambda own, number: shared_out(jax.random.fold_in(keys[1], 2), own, number, TOK_DEV, EXPERTS, TOP, CAP, 2))(routes_keys, routes_turns).reshape((TOKENS, TOP))
    route_weight = with_ends(jax.random.randint(keys[2], (TOKENS, TOP), 1, 4097), jax.random.fold_in(keys[2], 1), 1, 4096).astype(jnp.int32)
    w_gate = centred(keys[3], (EXPERTS, D, FF), D ** -0.5, 0.0625, ((0, 8), (2, 4)))
    w_up = centred(keys[4], (EXPERTS, D, FF), D ** -0.5, 0.0625, ((0, 8), (2, 4)))
    w_down = centred(keys[5], (EXPERTS, FF, D), FF ** -0.5, 0.125, ((0, 8), (1, 4)))
    prev_inputs = centred(keys[6], (N_DP, EXPERTS, PREV_ROWS, D), 1.0, 6.0, ((0, 4), (1, 8)))
    return {"tokens": tokens, "routes": routes, "route_weight": route_weight, "w_gate": w_gate, "w_up": w_up, "w_down": w_down, "prev_inputs": prev_inputs}


def route_slots(flat_ids):
    onehot = (flat_ids[:, None] == jnp.arange(EXPERTS, dtype=jnp.int32)[None, :]).astype(jnp.int32)
    earlier = jnp.cumsum(onehot, axis=0) - onehot
    return jnp.sum(earlier * onehot, axis=1).astype(jnp.int32)


def reference(tokens, routes, route_weight, w_gate, w_up, w_down, prev_inputs):
    blocks = routes.reshape(N_EXPERT, TOK_DEV * TOP).astype(jnp.int32)
    slots = jax.vmap(route_slots)(blocks)
    anchor = jnp.arange(N_EXPERT, dtype=jnp.int32)[:, None]
    places = ((blocks * N_EXPERT + anchor) * CAP + slots).astype(jnp.int32)
    token_ids = jnp.arange(TOKENS, dtype=jnp.int32).reshape(N_EXPERT, TOK_DEV, 1)
    token_ids = jnp.broadcast_to(token_ids, (N_EXPERT, TOK_DEV, TOP)).reshape(N_EXPERT, TOK_DEV * TOP)
    table = jnp.full((EXPERTS * N_EXPERT * CAP,), TOKENS, jnp.int32)
    table = table.at[places.reshape(-1)].set(token_ids.reshape(-1)).reshape(EXPERTS, N_EXPERT * CAP)
    padded = jnp.concatenate([tokens, jnp.zeros((1, D), tokens.dtype)], axis=0)
    slice_width = FF // N_DP

    def one_expert(item):
        index, gate_w, up_w, down_w = item
        rows = padded[index]
        gate = jnp.dot(rows, gate_w, preferred_element_type=jnp.float32)
        up = jnp.dot(rows, up_w, preferred_element_type=jnp.float32)
        hidden = (jax.nn.silu(gate) * up).astype(jnp.bfloat16)
        total = jnp.zeros((N_EXPERT * CAP, D), jnp.float32)
        for group in range(N_DP):
            piece = jnp.dot(hidden[:, group * slice_width:(group + 1) * slice_width],
                            down_w[group * slice_width:(group + 1) * slice_width],
                            preferred_element_type=jnp.float32).astype(jnp.bfloat16)
            total = total + lax.optimization_barrier(piece).astype(jnp.float32)
        return total

    outputs = lax.map(one_expert, (table, w_gate, w_up, w_down))
    flat_out = outputs.reshape(EXPERTS * N_EXPERT * CAP, D)
    picked = flat_out[places.reshape(-1)].reshape(TOKENS, TOP, D)
    counts = route_weight.astype(jnp.float32)
    shares = 2.5 * counts / jnp.sum(counts, axis=1, keepdims=True)
    mixed = jnp.sum(picked * shares[:, :, None], axis=1).astype(jnp.bfloat16)

    def one_gram(history):
        rows = history.reshape(N_DP * PREV_ROWS, D)
        gram = jnp.dot(rows.T, rows[:, :HESS_COLS], preferred_element_type=jnp.float32)
        return gram * (2.0 / (N_DP * PREV_ROWS))

    grams = lax.map(one_gram, jnp.moveaxis(prev_inputs, 1, 0))
    hessian = jnp.transpose(grams, (1, 0, 2))
    return mixed, hessian
```

```python
import jax
import jax.numpy as jnp
from jax import lax
from jax.sharding import PartitionSpec as P

HESS_COLS = 128
CORE, NEAR, FAR = 1, 2, 4


def swap(value, axis, bits):
    return lax.ppermute(value, axis, [(i, i ^ bits) for i in range(lax.axis_size(axis))])


def route_slots(flat_ids, experts_all):
    onehot = (flat_ids[:, None] == jnp.arange(experts_all, dtype=jnp.int32)[None, :]).astype(
        jnp.int32
    )
    earlier = jnp.cumsum(onehot, axis=0) - onehot
    return jnp.sum(earlier * onehot, axis=1)


def combine_rows(back, places, shares, tok_dev, top):
    columns = back.shape[-1]
    rows = back.reshape(-1, columns)[places]
    weighted = rows.astype(jnp.float32) * shares.reshape(-1, 1)
    return jnp.sum(weighted.reshape(tok_dev, top, columns), axis=1)


def routed(tokens, routes, route_weight, w_gate, w_up, w_down, prev_inputs):
    tok_dev, top = routes.shape
    exp_dev = w_gate.shape[0]
    width = tokens.shape[1]
    n_expert = lax.axis_size("expert")
    n_dp = lax.axis_size("dp")
    experts_all = exp_dev * n_expert
    capacity = min(tok_dev, tok_dev * top * 5 // (4 * experts_all))
    flat_ids = routes.reshape(-1)
    slots = route_slots(flat_ids, experts_all)
    places = flat_ids * capacity + slots
    weight_counts = route_weight.astype(jnp.float32)
    shares = 2.5 * weight_counts / jnp.sum(weight_counts, axis=1, keepdims=True)
    picks = jnp.arange(experts_all * capacity, dtype=jnp.int32)[:, None] == places[None, :]
    placing = jnp.any(picks.reshape(experts_all * capacity, tok_dev, top), axis=2).astype(
        jnp.bfloat16
    )
    outgoing = jnp.dot(placing, tokens, preferred_element_type=jnp.float32).astype(jnp.bfloat16)
    outgoing = outgoing.reshape(experts_all, capacity, width)
    arrived = lax.all_to_all(outgoing, "expert", split_axis=0, concat_axis=0, tiled=True)
    arrived = arrived.reshape(n_expert, exp_dev, capacity, width)
    gate = jnp.einsum("sjcd,jdf->sjcf", arrived, w_gate, preferred_element_type=jnp.float32)
    up = jnp.einsum("sjcd,jdf->sjcf", arrived, w_up, preferred_element_type=jnp.float32)
    history = prev_inputs.reshape(prev_inputs.shape[1], prev_inputs.shape[2], width)
    head_cols = history[:, :, :HESS_COLS]
    gram_scale = 2.0 / (n_dp * history.shape[1])
    hessian = lax.psum_scatter(
        (
            jnp.einsum("jrd,jrh->djh", history, head_cols, preferred_element_type=jnp.float32)
            * gram_scale
        ).astype(jnp.bfloat16),
        "dp",
        scatter_dimension=0,
        tiled=True,
    ).astype(jnp.float32)
    hidden = (jax.nn.silu(gate) * up).astype(jnp.bfloat16)
    partial_out = jnp.einsum("sjcf,jfd->sjcd", hidden, w_down, preferred_element_type=jnp.float32)
    partial_out = partial_out.astype(jnp.bfloat16)
    back = lax.all_to_all(
        partial_out.reshape(experts_all, capacity, width),
        "expert",
        split_axis=0,
        concat_axis=0,
        tiled=True,
    )
    own_sum = combine_rows(back, places, shares, tok_dev, top)
    mixed = lax.psum_scatter(own_sum.astype(jnp.bfloat16), "dp", scatter_dimension=1, tiled=True)
    return (mixed, hessian)


def group_columns(value, group, n_groups):
    size = value.shape[-1] // n_groups
    return lax.dynamic_slice_in_dim(value, group * size, size, axis=value.ndim - 1)


def window_hessian(history):
    n_dp = lax.axis_size("dp")
    here = lax.axis_index("dp")
    head = history[:, :HESS_COLS]

    def bundle(bits):
        return jnp.concatenate([group_columns(history, here ^ bits, n_dp), head], axis=1)

    bundles = [bundle(0)] + [swap(bundle(bits), "dp", bits) for bits in range(1, n_dp)]
    rows = jnp.concatenate(bundles, axis=0)
    columns, heads = rows[:, :-HESS_COLS], rows[:, -HESS_COLS:]
    gram = jnp.einsum("rd,rh->dh", columns, heads, preferred_element_type=jnp.float32)
    return (gram * (2.0 / rows.shape[0]))[:, None, :]


def shares_here(routes, route_weight, experts_all):
    counts = route_weight.astype(jnp.float32)
    shares = 2.5 * counts / jnp.sum(counts, axis=1, keepdims=True)
    named = routes[:, :, None] == jnp.arange(experts_all, dtype=jnp.int32)[None, None, :]
    table = jnp.sum(jnp.where(named, shares[:, :, None], 0.0), axis=1)
    tables = lax.all_gather(table.T, "expert", axis=0)
    me = lax.axis_index("expert")
    column = lax.dynamic_slice_in_dim(tables, me, 1, axis=1)[:, 0]
    return [
        lax.dynamic_slice_in_dim(column, me ^ bits, 1, axis=0)[0][:, None]
        for bits in range(experts_all)
    ]


def whole(tokens, routes, route_weight, w_gate, w_up, w_down, prev_inputs):
    tok_dev, top = routes.shape
    width = tokens.shape[1]
    half = tok_dev // 2
    n_dp = lax.axis_size("dp")
    w_gate, w_up, w_down = w_gate[0], w_up[0], w_down[0]
    share = shares_here(routes, route_weight, top)
    near = swap(tokens, "expert", NEAR)
    far = swap(tokens, "expert", FAR)
    hessian = window_hessian(prev_inputs.reshape(prev_inputs.shape[2], width))
    tokens_c = swap(tokens, "expert", CORE)
    corner = jnp.concatenate(
        [swap(far[:half], "expert", NEAR), swap(near[half:], "expert", FAR)], axis=0
    )
    near_c, far_c, corner_c = (swap(v, "expert", CORE) for v in (near, far, corner))

    def hidden_of(blocks, bits):
        x = jnp.concatenate(blocks, axis=0)
        gate = jnp.dot(x, w_gate, preferred_element_type=jnp.float32)
        up = jnp.dot(x, w_up, preferred_element_type=jnp.float32)
        scale = jnp.concatenate([share[b] for b in bits], axis=0)
        rows = (jax.nn.silu(gate) * up * scale).astype(jnp.bfloat16)
        return dict(zip(bits, jnp.split(rows, len(bits), axis=0)))

    early = hidden_of(
        [tokens, tokens_c, near, near_c, far, far_c], [0, CORE, NEAR, NEAR ^ CORE, FAR, FAR ^ CORE]
    )
    late = hidden_of([corner, corner_c], [NEAR ^ FAR, NEAR ^ FAR ^ CORE])
    hidden = early | late

    def rows_of(low, high, flip):
        return jnp.concatenate(
            [hidden[b ^ flip][:half] for b in low] + [hidden[b ^ flip][half:] for b in high], axis=0
        )

    def down(rows, added=None):
        out = jnp.dot(rows, w_down, preferred_element_type=jnp.float32)
        if added is not None:
            out = out + added.astype(jnp.float32)
        return out.astype(jnp.bfloat16)

    leaving = ((NEAR, NEAR ^ FAR), (FAR, NEAR ^ FAR))
    staying = ((0, FAR), (0, NEAR))
    leaving_c = swap(down(rows_of(*leaving, CORE)), "expert", CORE)
    staying_c = swap(down(rows_of(*staying, CORE)), "expert", CORE)
    first = down(rows_of(*leaving, 0), leaving_c)
    got_low = swap(first[:tok_dev], "expert", NEAR)
    got_high = swap(first[tok_dev:], "expert", FAR)
    second = down(rows_of(*staying, 0), staying_c)

    def add(a, b):
        return (a.astype(jnp.float32) + b.astype(jnp.float32)).astype(jnp.bfloat16)

    low = second[:tok_dev]
    high = second[tok_dev:]
    last_low = swap(add(got_low[half:], low[half:]), "expert", FAR)
    last_high = swap(add(got_high[half:], high[half:]), "expert", NEAR)
    plane = jnp.concatenate(
        [
            got_low[:half].astype(jnp.float32) + low[:half] + last_low,
            got_high[:half].astype(jnp.float32) + high[:half] + last_high,
        ],
        axis=0,
    ).astype(jnp.bfloat16)
    here = lax.axis_index("dp")
    mixed = group_columns(plane, here, n_dp).astype(jnp.float32)
    for bits in range(1, n_dp):
        mixed = mixed + swap(group_columns(plane, here ^ bits, n_dp), "dp", bits).astype(jnp.float32)
    return (mixed.astype(jnp.bfloat16), hessian)


def solution(mesh):
    placed = (
        P("expert", None),
        P("expert", None),
        P("expert", None),
        P("expert", None, "dp"),
        P("expert", None, "dp"),
        P("expert", "dp", None),
        P("dp", "expert", None, None),
    )

    def shards(*args):
        routes, w_gate = args[1], args[3]
        n_expert, n_dp = mesh.shape["expert"], mesh.shape["dp"]
        every = routes.shape[1] == n_expert * w_gate.shape[0] and w_gate.shape[0] == 1
        if every and n_expert == CORE + NEAR + FAR + 1 and n_dp & (n_dp - 1) == 0:
            return whole(*args)
        return routed(*args)

    return jax.shard_map(
        shards,
        mesh=mesh,
        in_specs=placed,
        out_specs=(P("expert", "dp"), P("dp", "expert", None)),
        check_vma=False,
    )
```
